128 devices in a mesh: expert: 8 (over y, core), mp: 16 (over z, x).
Axes of the slice: x: 4, y: 4, z: 4, core: 2. Of those that a mesh axis runs over, the one named last changes fastest.
Arguments:
- tokens: bfloat16 [2048, 6144], P(('expert', 'mp')), may hold values from -18 to 18
- norm_gain: bfloat16 [6144], replicated, may hold values from 0.099609375 to 1.8984375
- expert_ids: int32 [2048, 2], P(('expert', 'mp')), may hold values from 0 to 7, as said below
- slot_ids: int32 [2048, 2], P(('expert', 'mp')), may hold values from 0 to 7, as said below
- route_weights: float32 [2048, 2], P(('expert', 'mp')), may hold values from 0.1 to 1
- w_gate: bfloat16 [8, 6144, 8192], P('expert', None, 'mp'), may hold values from -0.078125 to 0.078125
- w_up: bfloat16 [8, 6144, 8192], P('expert', None, 'mp'), may hold values from -0.078125 to 0.078125
- w_down: bfloat16 [8, 8192, 6144], P('expert', 'mp'), may hold values from -0.0625 to 0.0625
Outputs:
- moe_out: bfloat16 [2048, 6144], P(('expert', 'mp'))
The draws below stay inside these ranges and needn't reach their ends.
Inputs may be any that keep to these rules, and one draw needn't show every extreme that they name: `expert_ids`: each token names two different experts. Among the 16 tokens of one device (aligned blocks of rows) no expert is named more than 8 times, and on every device some expert is named exactly 8 times. `slot_ids`: within the tokens of one device, the entries that name the same expert have different slots; slots that no entry names stay empty.
All inputs are finite; a program needn't handle non-finite values.
Results may differ from the reference program's by a relative error of at most 0.015.
Values may be sent and summed in bfloat16 or wider, within the bound.
A program may use at most 128 MiB of HBM per device.

```python
import math
import jax
import jax.numpy as jnp
from jax import lax

D = 6144
FF = 8192
EXPERTS = 8
TOK_DEV = 16
CAP = 8
TOKENS = 2048
N_MP = 16


def route_tables(key):
    blocks = TOKENS // TOK_DEV

    def one_block(index):
        block_key = jax.random.fold_in(key, index)
        key_busy, key_pool, key_slot, key_order = jax.random.split(block_key, 4)
        busiest = jax.random.randint(key_busy, (), 0, EXPERTS)
        labels = jnp.arange((EXPERTS - 1) * CAP, dtype=jnp.int32) // CAP
        others = labels + (labels >= busiest).astype(jnp.int32)
        mixing = jax.random.permutation(key_pool, (EXPERTS - 1) * CAP)
        chosen = others[mixing[:2 * TOK_DEV - CAP]]
        sequence = jnp.sort(jnp.concatenate([jnp.full((CAP,), busiest, jnp.int32), chosen]))
        below = jnp.sum((sequence[None, :] < sequence[:, None]).astype(jnp.int32), axis=1)
        within = jnp.arange(2 * TOK_DEV, dtype=jnp.int32) - below
        tables = jax.vmap(lambda expert: jax.random.permutation(jax.random.fold_in(key_slot, expert), CAP))(jnp.arange(EXPERTS))
        slot_sequence = tables[sequence, within].astype(jnp.int32)
        token_order = jax.random.permutation(key_order, TOK_DEV)
        chosen_ids = jnp.stack([sequence[token_order], sequence[TOK_DEV + token_order]], axis=1)
        chosen_slots = jnp.stack([slot_sequence[token_order], slot_sequence[TOK_DEV + token_order]], axis=1)
        return (chosen_ids, chosen_slots)
    all_ids, all_slots = jax.vmap(one_block)(jnp.arange(blocks))
    return (all_ids.reshape(TOKENS, 2).astype(jnp.int32), all_slots.reshape(TOKENS, 2).astype(jnp.int32))


def draw_expert_ids(key, part):
    return route_tables(jax.random.fold_in(key, 7))[0]


def draw_slot_ids(key, part):
    return route_tables(jax.random.fold_in(key, 7))[1]


def draw_tokens(key, part):
    key_base, key_scale = jax.random.split(jax.random.fold_in(key, 3))
    base = jnp.clip(jax.random.normal(key_base, (TOKENS, D), jnp.float32), -6.0, 6.0)
    scale = jnp.exp(jax.random.uniform(key_scale, (TOKENS, 1), jnp.float32, math.log(0.3), math.log(3.0)))
    return (base * scale).astype(jnp.bfloat16)


def steps_of(own_key, dims, shards, least, largest):
    factor_of, own = 1.0, jax.random.fold_in(own_key, 6)
    for axis_at, parts in shards:
        steps = jnp.exp(jax.random.uniform(jax.random.fold_in(own, axis_at), (parts,), jnp.float32, least / len(shards), largest / len(shards)))
        factor_of = factor_of * jnp.repeat(steps, dims[axis_at] // parts).reshape([-1 if axis == axis_at else 1 for axis in range(len(dims))])
    return factor_of


def normal_values(rng, extent, scale, bound, shards=(), held_as=jnp.bfloat16):
    gain = steps_of(rng, extent, shards, -0.22, 0.18) if shards else 1.0
    entries = jax.random.normal(rng, extent, jnp.float32) * scale * gain
    return jnp.minimum(jnp.maximum(entries, -bound), bound).astype(held_as)


def setup_inputs(seed: int = 0) -> dict:
    key_of = jax.random.split(jax.random.key(seed), 9)
    return {
        "tokens": draw_tokens(jax.random.fold_in(key_of[8], 71), 0),
        "norm_gain": jnp.clip(1.0 + 0.18 * jax.random.normal(key_of[1], (D,), jnp.float32), 0.099609375, 1.8984375).astype(jnp.bfloat16),
        "expert_ids": draw_expert_ids(jax.random.fold_in(key_of[8], 71), 0),
        "slot_ids": draw_slot_ids(jax.random.fold_in(key_of[8], 71), 0),
        "route_weights": jnp.clip(jnp.exp(math.log(1.0) - 2.3025851 * jax.random.uniform(key_of[4], (TOKENS, 2), jnp.float32) ** steps_of(key_of[4], (TOKENS, 2), ((0, 128),), -0.2, 0.2)), 0.1, 1.0),
        "w_gate": normal_values(key_of[5], (EXPERTS, D, FF), D ** -0.5, 0.078125, ((0, 8), (2, 16))),
        "w_up": normal_values(key_of[6], (EXPERTS, D, FF), D ** -0.5, 0.078125, ((0, 8), (2, 16))),
        "w_down": normal_values(key_of[7], (EXPERTS, FF, D), FF ** -0.5, 0.0625, ((0, 8), (1, 16))),
    }


def reference(tokens, norm_gain, expert_ids, slot_ids, route_weights, w_gate, w_up, w_down):
    values = tokens.astype(jnp.float32)
    mean_square = lax.optimization_barrier(jnp.mean(values * values, axis=1, keepdims=True))
    normed = (values * lax.rsqrt(mean_square + 1e-05) * norm_gain.astype(jnp.float32)).astype(jnp.bfloat16)
    block_index = (jnp.arange(TOKENS, dtype=jnp.int32) // TOK_DEV).astype(jnp.int32)
    row_index = (block_index[:, None] * CAP + slot_ids).astype(jnp.int32)
    expert_rows = TOKENS // TOK_DEV * CAP
    buffer = jnp.zeros((EXPERTS, expert_rows, D), jnp.bfloat16)
    filled = jnp.broadcast_to(normed[:, None, :], (TOKENS, 2, D))
    buffer = buffer.at[expert_ids, row_index].set(filled)
    share_width = FF // N_MP

    def one_expert(operands):
        block, gate_mat, up_mat, down_mat = operands
        gate_proj = jnp.dot(block, gate_mat, preferred_element_type=jnp.float32)
        up_proj = jnp.dot(block, up_mat, preferred_element_type=jnp.float32)
        hidden = (jax.nn.silu(gate_proj) * up_proj).astype(jnp.bfloat16)

        def add_share(total, index):
            first = (index * share_width).astype(jnp.int32)
            part_hidden = lax.dynamic_slice_in_dim(hidden, first, share_width, 1)
            part_down = lax.dynamic_slice_in_dim(down_mat, first, share_width, 0)
            product = jnp.dot(part_hidden, part_down, preferred_element_type=jnp.float32).astype(jnp.bfloat16)
            product = lax.optimization_barrier(product)
            return (total + product.astype(jnp.float32), None)
        start_total = jnp.zeros((expert_rows, D), jnp.float32)
        total, unused = lax.scan(add_share, start_total, jnp.arange(N_MP, dtype=jnp.int32))
        return total.astype(jnp.bfloat16)
    expert_out = lax.map(one_expert, (buffer, w_gate, w_up, w_down))
    shares = route_weights / (route_weights[:, 0:1] + route_weights[:, 1:2])
    picked = expert_out[expert_ids, row_index].astype(jnp.float32)
    mixed = lax.optimization_barrier(jnp.sum(shares[:, :, None] * picked, axis=1))
    return mixed.astype(jnp.bfloat16)
```

```python
import jax
import jax.numpy as jnp
from jax import lax
from jax.experimental import pallas as pl
from jax.experimental.pallas import tpu as pltpu
from jax.sharding import PartitionSpec as P

MESH = pl.DeviceIdType.MESH
D = 6144
PW = 2048
HW = 1024
EXT = 128
F = 512
ORDER = ((2, 1, 0), (1, 0, 2), (0, 2, 1))
REL = (0, -1, 1, 2)
RS_SUB = (2, 1, -1, 0)

RATE = 46600.0 * 0.93
LAT = 2.4
T_MM = 1.35
T_DN = 1.4
T_EV = 0.1


def plan_gather():
    t = 3.0
    free, arrive, order = {}, [], []
    done, sent = set(), set()
    weight_ready = {(0, 0): 5.0, (1, 0): 7.0, (2, 0): 9.0, (0, 1): 14.0, (1, 1): 22.0, (2, 1): 30.0}
    items = [(p, r, j) for j in (0, 1) for r in REL for p in range(3)]

    def send(p, s, k):
        ax = ORDER[p][0 if s == 0 else (1 if s < 5 else 2)]
        size = (65536 if s < 5 else 262144) // (1 if k < 2 else 2)
        if p == 2:
            size = size * 17 // 16
        way = k % 2
        begin = max(free.get((ax, way), 0.0), t)
        free[ax, way] = begin + size / RATE
        arrive.append((free[ax, way] + LAT, p, s, k))
        order.append(("send", p, s, k))

    def ready(p, s):
        got = lambda q, ks: all((p, q, k) in done for k in ks)
        if s == 0:
            return True
        if s < 5:
            return got(0, ((), (0,), (1,), (2, 3))[s - 1])
        ks = ((), (0,), (1,), (2, 3))[s - 5]
        if s == 5:
            return got(0, (0, 1, 2, 3))
        return all(got(q, ks) for q in (1, 2, 3, 4))

    def pump():
        for s in range(9):
            for p in range(3):
                if (p, s) not in sent and ready(p, s):
                    sent.add((p, s))
                    send(p, s, 0)
                    send(p, s, 1)

    def plane_ready(p, r):
        if r == 0:
            return all((p, s, k) in done for s in range(5) for k in range(4))
        ks = {-1: (0,), 1: (1,), 2: (2, 3)}[r]
        return all((p, s, k) in done for s in (5, 6, 7, 8) for k in ks)

    pump()
    while arrive or items:
        arrive.sort()
        ripe = [i for i in items if plane_ready(i[0], i[1]) and (weight_ready[i[0], i[2]] <= t or not arrive)]
        if arrive and (arrive[0][0] <= t or not ripe):
            at, p, s, k = arrive.pop(0)
            t = max(t, at) + T_EV
            done.add((p, s, k))
            order.append(("recv", p, s, k))
            if k < 2:
                send(p, s, k + 2)
            pump()
        else:
            item = ripe[0]
            items.remove(item)
            order.append(("mm",) + item)
            t += T_MM
    return order, t


def plan_scatter():
    t = 0.0
    free, arrive, order = {}, [], []
    done = set()
    items = [("dn", p, r) for r in (2, 1, -1, 0) for p in range(3)]
    todo = []
    for p in range(3):
        for st in (1, 2, 3):
            ax = ORDER[p][3 - st]
            rows = {1: 64, 2: 64, 3: 16}[st]
            size = rows * HW * 2
            for v in RS_SUB if st == 1 else (0,):
                def have(r, st=st, v=v, p=p):
                    if st == 1:
                        return ("dn", p, r)
                    if st == 2:
                        return ("own", p, 1, r)
                    return ("own", p, 2, 0)
                todo.append(((have(2),), ("rsend", p, st, v, 0, 0), ax, size))
                todo.append(((have(2),), ("rsend", p, st, v, 1, 0), ax, size))
                todo.append(((have(1),), ("rsend", p, st, v, 0, 1), ax, size))
                todo.append(((have(-1),), ("rsend", p, st, v, 1, 1), ax, size))
                todo.append(((have(1), ("rrecv", p, st, v, 0, 0)), ("rsend", p, st, v, 0, 2), ax, size))
                todo.append(((have(-1), ("rrecv", p, st, v, 1, 0)), ("rsend", p, st, v, 1, 2), ax, size))
                todo.append((
                    (have(0),) + tuple(("rrecv", p, st, v, w, q) for w in (0, 1) for q in (1, 2)),
                    ("own", p, st, v), None, 0,
                ))

    def pump():
        moved = True
        while moved:
            moved = False
            for entry in list(todo):
                needs, op, ax, size = entry
                if all(n in done for n in needs):
                    todo.remove(entry)
                    order.append(op)
                    if op[0] == "rsend":
                        _, p, st, v, way, kind = op
                        begin = max(free.get((ax, way), 0.0), t)
                        free[ax, way] = begin + size / RATE
                        arrive.append((free[ax, way] + LAT, ("rrecv", p, st, v, way, kind)))
                    else:
                        done.add(op)
                    moved = True
                    break

    while arrive or items or todo:
        arrive.sort()
        if arrive and (arrive[0][0] <= t or not items):
            at, op = arrive.pop(0)
            t = max(t, at) + T_EV
            done.add(op)
            order.append(op)
        else:
            item = items.pop(0)
            order.append(item)
            t += T_DN
            done.add(item)
        pump()
    return order, t


def kernel(
    tok, gain, ids, rw, wg, wu, wd, out, wdp,
    w0, w1, w2, g, acc, h, r1a, r1b, r2a, r2b, r3a, r3b,
    gs_sem, gr_sem, rs_sem, rr_sem, wl_sem, ws_sem, wr_sem, dl_sem,
):
    ws = (w0, w1, w2)
    ex, mp = lax.axis_index("expert"), lax.axis_index("mp")
    core, cy = lax.rem(ex, 2), lax.div(ex, 2)
    cx, cz = lax.rem(mp, 4), lax.div(mp, 4)
    me = (cz, cy, cx)
    pos = [[me[ax] if r == 0 else lax.rem(me[ax] + (r + 4) % 4, 4) for r in (0, 1, 2, -1)] for ax in range(3)]

    def at(ax, r):
        return pos[ax][r]

    def dev(ax, r):
        cc = [at(q, r if q == ax else 0) for q in range(3)]
        return (cc[1] * 2 + core, cc[0] * 4 + cc[2])

    other_core = (cy * 2 + (1 - core), mp)

    bar = pltpu.get_barrier_semaphore()
    for ax in range(3):
        for r in (1, -1):
            pl.semaphore_signal(bar, inc=1, device_id=dev(ax, r), device_id_type=MESH)
    pl.semaphore_signal(bar, inc=1, device_id=other_core, device_id_type=MESH)

    local_w = []
    for p in range(3):
        for q, src in ((0, wg), (1, wu)):
            cp = pltpu.make_async_copy(src.at[p], ws[p].at[:, :, :, :, :, pl.ds(q * F, F)], wl_sem.at[p, q])
            cp.start()
            local_w.append(cp)

    vals = tok[...].astype(jnp.float32)
    ms = jnp.mean(vals * vals, axis=1, keepdims=True)
    normed = (vals * lax.rsqrt(ms + 1e-05) * gain[...].astype(jnp.float32)).astype(jnp.bfloat16)
    g[cz, cy, cx, :, pl.ds(0, D)] = normed
    lane = lax.broadcasted_iota(jnp.int32, (16, EXT), 1)
    weights = rw[...]
    share = weights / (weights[:, 0:1] + weights[:, 1:2])
    which = ids[...]
    name = lax.rem(lane, 8)
    coef = jnp.where(name == which[:, 0:1], share[:, 0:1], 0.0) + jnp.where(name == which[:, 1:2], share[:, 1:2], 0.0)
    hi = coef.astype(jnp.bfloat16).astype(jnp.float32)
    packed = jnp.where(lane < 8, hi, jnp.where(lane < 16, coef - hi, 0.0))
    g[cz, cy, cx, :, pl.ds(D, EXT)] = packed.astype(jnp.bfloat16)

    pl.semaphore_wait(bar, 7)

    def region(p, s, r, half):
        a, b, c = ORDER[p]
        idx = [None, None, None]
        if s == 0:
            idx[a], idx[b], idx[c] = at(a, r), at(b, 0), at(c, 0)
        elif s < 5:
            idx[a], idx[b], idx[c] = at(a, REL[s - 1]), at(b, r), at(c, 0)
        else:
            idx[a], idx[b], idx[c] = slice(None), at(b, REL[s - 5]), at(c, r)
        lo, hi_ = p * PW, (p + 1) * PW + (EXT if p == 2 else 0)
        if half == 0:
            hi_ = lo + HW
        elif half == 1:
            lo = lo + HW
        return g.at[idx[0], idx[1], idx[2], :, pl.ds(lo, hi_ - lo)]

    def gcopy(p, s, k, sending):
        way = 1 if k % 2 == 0 else -1
        if sending:
            r = 0 if k < 2 else -way
        else:
            r = -way if k < 2 else 2
        reg = region(p, s, r, None if k < 2 else k - 2)
        ax = ORDER[p][0 if s == 0 else (1 if s < 5 else 2)]
        return pltpu.make_async_remote_copy(
            src_ref=reg, dst_ref=reg, send_sem=gs_sem.at[p, s, k], recv_sem=gr_sem.at[p, s, k],
            device_id=dev(ax, way), device_id_type=MESH,
        )

    def wcopy(p, q):
        src = (wg, wu)[q]
        return pltpu.make_async_remote_copy(
            src_ref=src.at[p], dst_ref=ws[p].at[:, :, :, :, :, pl.ds(2 * F + q * F, F)],
            send_sem=ws_sem.at[p, q], recv_sem=wr_sem.at[p, q], device_id=other_core, device_id_type=MESH,
        )

    dcopy = pltpu.make_async_remote_copy(
        src_ref=wd, dst_ref=wdp, send_sem=ws_sem.at[3, 0], recv_sem=wr_sem.at[3, 0],
        device_id=other_core, device_id_type=MESH,
    )

    def plane(ax, r):
        return tuple(at(ax, r) if q == ax else slice(None) for q in range(3))

    def mm(p, r, j):
        z, y, x = plane(ORDER[p][2], r)

        def tile(n, carry):
            cols = pl.ds(pl.multiple_of(j * 2 * F + n * F, F), F)
            lhs = g[z, y, x, :, pl.ds(p * PW, PW)].reshape(256, PW)
            rhs = ws[p][:, :, :, :, :, cols].reshape(PW, F)
            res = jnp.dot(lhs, rhs, preferred_element_type=jnp.float32)
            acc[z, y, x, :, cols] += res.reshape(4, 4, 16, F)
            return carry

        lax.fori_loop(0, 2, tile, 0)

    gather, _ = plan_gather()
    started = False
    have_w = set()
    acc[...] = jnp.zeros_like(acc)
    for op in gather:
        if op[0] == "send":
            gcopy(*op[1:], True).start()
        elif op[0] == "recv":
            if not started:
                started = True
                for p in range(3):
                    for q in range(2):
                        wcopy(p, q).start()
                dcopy.start()
            gcopy(*op[1:], False).wait_recv()
        else:
            _, p, r, j = op
            if (p, j) not in have_w:
                have_w.add((p, j))
                for q in range(2):
                    if j == 0:
                        local_w[p * 2 + q].wait()
                    else:
                        wcopy(p, q).wait_recv()
            mm(p, r, j)

    dcopy.wait_recv()
    down = []
    for p in range(3):
        for q, src in ((0, wd), (1, wdp)):
            cp = pltpu.make_async_copy(
                src.at[:, :, :, :, pl.ds(p * PW, PW)], ws[p].at[0, pl.ds(2 * q, 2)], dl_sem.at[p, q]
            )
            cp.start()
            down.append(cp)

    e_of = (ex, cy * 2 + (1 - core))

    def act(i, carry):
        z, y = lax.div(i, 4), lax.rem(i, 4)
        tile = g[z, y, :, :, pl.ds(D, EXT)].reshape(64, EXT).astype(jnp.float32)
        ln = lax.broadcasted_iota(jnp.int32, (64, EXT), 1)
        for j in range(2):
            mine = jnp.where((ln == e_of[j]) | (ln == e_of[j] + 8), tile, 0.0)
            cf = jnp.sum(mine, axis=1, keepdims=True)
            gate = acc[z, y, :, :, pl.ds(j * 2 * F, F)].reshape(64, F)
            up = acc[z, y, :, :, pl.ds(j * 2 * F + F, F)].reshape(64, F)
            res = gate / (1.0 + jnp.exp(-gate)) * up * cf
            h[z, y, :, :, pl.ds(j * F, F)] = res.astype(jnp.bfloat16).reshape(4, 16, F)
        return carry

    lax.fori_loop(0, 16, act, 0)

    def dn(p, r):
        z, y, x = plane(ORDER[p][2], r)

        def tile(n, carry):
            cols = pl.ds(pl.multiple_of(n * F, F), F)
            lhs = h[z, y, x].reshape(256, 2 * F)
            rhs = ws[p][0, :, :, :, :, cols].reshape(2 * F, F)
            res = jnp.dot(lhs, rhs, preferred_element_type=jnp.float32)
            ws[p][1, z, y, x, :, cols] = res.astype(jnp.bfloat16).reshape(4, 4, 16, F)
            return carry

        lax.fori_loop(0, PW // F, tile, 0)

    def part_region(p, st, v, r):
        a, b, c = ORDER[p]
        idx = [None, None, None]
        if st == 1:
            idx[a], idx[b], idx[c] = slice(None), at(b, v), at(c, r)
        elif st == 2:
            idx[a], idx[b], idx[c] = slice(None), at(b, r), at(c, 0)
        else:
            idx[a], idx[b], idx[c] = at(a, r), at(b, 0), at(c, 0)
        return tuple(idx)

    def half_cols(half):
        return pl.ds(half * HW, HW)

    def bufs(p, st, v, way):
        i = RS_SUB.index(v)
        if st == 1:
            return r1a.at[p, way, i], r1b.at[p, way, i]
        if st == 2:
            return r2a.at[p, way], r2b.at[p, way]
        return r3a.at[p, way], r3b.at[p, way]

    def slot(st, v):
        return RS_SUB.index(v) if st == 1 else st + 2

    def rcopy(p, st, v, way, kind):
        step = 1 if way == 0 else -1
        r = 2 if kind == 0 else step
        half = way if kind in (0, 2) else 1 - way
        z, y, x = part_region(p, st, v, r)
        src = ws[p].at[1, z, y, x, :, half_cols(half)]
        buf_a, buf_b = bufs(p, st, v, way)
        if kind == 0:
            dst = buf_a
        elif st == 3:
            dst = buf_b.at[:, half_cols(half)]
        else:
            dst = buf_b.at[:, :, half_cols(half)]
        return pltpu.make_async_remote_copy(
            src_ref=src, dst_ref=dst, send_sem=rs_sem.at[p, slot(st, v), way, kind],
            recv_sem=rr_sem.at[p, slot(st, v), way, kind],
            device_id=dev(ORDER[p][3 - st], step), device_id_type=MESH,
        )

    scatter, _ = plan_scatter()
    have_d = set()
    for op in scatter:
        if op[0] == "dn":
            _, p, r = op
            if p not in have_d:
                have_d.add(p)
                down[2 * p].wait()
                down[2 * p + 1].wait()
            dn(p, r)
        elif op[0] == "rsend":
            _, p, st, v, way, kind = op
            if kind == 2:
                z, y, x = part_region(p, st, v, 1 if way == 0 else -1)
                buf_a, _ = bufs(p, st, v, way)
                cols = half_cols(way)
                total = ws[p][1, z, y, x, :, cols].astype(jnp.float32) + buf_a[...].astype(jnp.float32)
                ws[p][1, z, y, x, :, cols] = total.astype(jnp.bfloat16)
            rcopy(p, st, v, way, kind).start()
        elif op[0] == "rrecv":
            rcopy(*op[1:]).wait_recv()
        else:
            _, p, st, v = op
            z, y, x = part_region(p, st, v, 0)
            b0, b1 = bufs(p, st, v, 0)[1], bufs(p, st, v, 1)[1]
            total = (
                ws[p][1, z, y, x].astype(jnp.float32) + b0[...].astype(jnp.float32) + b1[...].astype(jnp.float32)
            ).astype(jnp.bfloat16)
            if st == 3:
                out[:, pl.ds(p * PW, PW)] = total
            else:
                ws[p][1, z, y, x] = total

    for op in gather:
        if op[0] == "send":
            gcopy(*op[1:], True).wait_send()
    for op in scatter:
        if op[0] == "rsend":
            rcopy(*op[1:]).wait_send()
    for p in range(3):
        for q in range(2):
            wcopy(p, q).wait_send()
    dcopy.wait_send()


def local(tokens, norm_gain, expert_ids, slot_ids, route_weights, w_gate, w_up, w_down):
    bf = jnp.bfloat16
    vmem = pl.BlockSpec(memory_space=pltpu.VMEM)
    hbm = pl.BlockSpec(memory_space=pl.ANY)
    moe, _ = pl.pallas_call(
        kernel,
        name="moe",
        out_shape=(
            jax.ShapeDtypeStruct((16, D), bf),
            jax.ShapeDtypeStruct((2, 4, 4, 16, D), bf),
        ),
        in_specs=[vmem, vmem, vmem, vmem, hbm, hbm, hbm],
        out_specs=(vmem, hbm),
        scratch_shapes=[
            pltpu.VMEM((2, 4, 4, 4, 16, PW), bf),
            pltpu.VMEM((2, 4, 4, 4, 16, PW), bf),
            pltpu.VMEM((2, 4, 4, 4, 16, PW), bf),
            pltpu.VMEM((4, 4, 4, 16, D + EXT), bf),
            pltpu.VMEM((4, 4, 4, 16, 4 * F), jnp.float32),
            pltpu.VMEM((4, 4, 4, 16, 2 * F), bf),
            pltpu.VMEM((3, 2, 4, 4, 16, HW), bf),
            pltpu.VMEM((3, 2, 4, 4, 16, PW), bf),
            pltpu.VMEM((3, 2, 4, 16, HW), bf),
            pltpu.VMEM((3, 2, 4, 16, PW), bf),
            pltpu.VMEM((3, 2, 16, HW), bf),
            pltpu.VMEM((3, 2, 16, PW), bf),
            pltpu.SemaphoreType.DMA((3, 9, 4)),
            pltpu.SemaphoreType.DMA((3, 9, 4)),
            pltpu.SemaphoreType.DMA((3, 6, 2, 3)),
            pltpu.SemaphoreType.DMA((3, 6, 2, 3)),
            pltpu.SemaphoreType.DMA((3, 2)),
            pltpu.SemaphoreType.DMA((4, 2)),
            pltpu.SemaphoreType.DMA((4, 2)),
            pltpu.SemaphoreType.DMA((3, 2)),
        ],
        compiler_params=pltpu.CompilerParams(
            collective_id=0, has_side_effects=True, vmem_limit_bytes=67043328
        ),
    )(
        tokens,
        norm_gain.reshape(1, D),
        expert_ids,
        route_weights,
        w_gate.reshape(3, 2, 4, 4, 4, 16, F),
        w_up.reshape(3, 2, 4, 4, 4, 16, F),
        w_down.reshape(2, 4, 4, 16, D),
    )
    return moe


def solution(mesh):
    placed = (
        P(("expert", "mp"), None),
        P(),
        P(("expert", "mp"), None),
        P(("expert", "mp"), None),
        P(("expert", "mp"), None),
        P("expert", None, "mp"),
        P("expert", None, "mp"),
        P("expert", "mp", None),
    )
    return jax.shard_map(
        local, mesh=mesh, in_specs=placed, out_specs=P(("expert", "mp"), None), check_vma=False
    )
```

```python
import jax
import jax.numpy as jnp
from jax import lax
from jax.experimental import pallas as pl
from jax.experimental.pallas import tpu as pltpu
from jax.sharding import PartitionSpec as P

MESH = pl.DeviceIdType.MESH
D = 6144
PW = 2048
HW = 1024
EXT = 128
F = 512
ORDER = ((2, 1, 0), (1, 0, 2), (0, 2, 1))
REL = (0, -1, 1, 2)
RS_SUB = (2, 1, -1, 0)

RATE = 46600.0 * 0.98
LAT = 2.0
T_MM = 1.15
T_DN = 1.1
T_EV = 0.06
WEIGHT = ((5.0, 6.0, 7.0), (14.0, 20.0, 26.0))


def axis_of(s):
    return 0 if s == 0 else (1 if s < 5 else 2)


def plan_gather():
    t = 2.0
    free, arrive, order = {}, [], []
    done, sent, held = set(), set(), {}
    weight_ready = {(p, j): WEIGHT[j][p] for p in range(3) for j in range(2)}
    passes = [(p, n, j) for n in range(4) for j in (0, 1) for p in range(3)]

    def put(p, s, k):
        size = (65536 if s < 9 else 262144) // (1 if k < 2 else 2)
        if p == 2:
            size = size * 17 // 16
        link = (ORDER[p][axis_of(s)], k % 2)
        begin = max(free.get(link, 0.0), t)
        free[link] = begin + size / RATE
        arrive.append((free[link] + LAT, p, s, k))
        order.append(("send", p, s, k))

    def send(p, s, k):
        if k > 1 and s >= 5 and not all((p, q) in sent for q in range(5, 12)):
            held.setdefault(p, []).append((p, s, k))
        else:
            put(p, s, k)

    def ready(p, s):
        got = lambda q, ks: all((p, q, k) in done for k in ks)
        if s == 0:
            return True
        if s < 9:
            return got(0, ((), (0,), (1,), (2, 3))[(s - 1) % 4])
        return all(got(q, ((0,), (1,), (2, 3))[s - 9]) for q in (1, 2, 3, 4))

    def pump():
        for s in range(12):
            for p in range(3):
                if (p, s) not in sent and ready(p, s):
                    sent.add((p, s))
                    send(p, s, 0)
                    send(p, s, 1)
        for p in range(3):
            if p in held and all((p, q) in sent for q in range(5, 12)):
                for entry in held.pop(p):
                    put(*entry)

    def ripe(p, n, j):
        if n == 0:
            ok = all((p, s, k) in done for s in range(5) for k in range(4))
        elif n == 1:
            ok = all((p, s, k) in done for s in range(5, 10) for k in range(2))
        elif n == 2:
            ok = all((p, s, k) in done for s in (10, 11) for k in range(2))
        else:
            ok = all((p, s, k) in done for s in range(5, 12) for k in (2, 3))
        return ok and (weight_ready[p, j] <= t or not arrive)

    pump()
    last = None
    while arrive or passes:
        arrive.sort()
        now = [i for i in passes if ripe(*i)]
        if arrive and (arrive[0][0] <= t or not now):
            at, p, s, k = arrive.pop(0)
            t = max(t, at) + T_EV
            done.add((p, s, k))
            order.append(("recv", p, s, k))
            if k < 2:
                send(p, s, k + 2)
            pump()
            if not arrive:
                last = t
        else:
            if not arrive:
                now.sort(key=lambda i: (i[0], i[1], i[2]))
            item = now[0]
            passes.remove(item)
            order.append(("mm",) + item)
            if not any(i[0] == item[0] for i in passes):
                order.append(("wd", item[0]))
            t += T_MM
    return order, t, last


def plan_scatter():
    t = 0.0
    free, arrive, order = {}, [], []
    done = set()
    items = [("dn", p, r) for r in (2, 1, -1, 0) for p in range(3)]
    todo = []
    for p in range(3):
        for st in (1, 2, 3):
            ax = ORDER[p][3 - st]
            rows = {1: 64, 2: 64, 3: 16}[st]
            size = rows * HW * 2
            for v in RS_SUB if st == 1 else (0,):
                def have(r, st=st, v=v, p=p):
                    if st == 1:
                        return ("dn", p, r)
                    if st == 2:
                        return ("own", p, 1, r)
                    return ("own", p, 2, 0)
                todo.append(((have(2),), ("rsend", p, st, v, 0, 0), ax, size))
                todo.append(((have(2),), ("rsend", p, st, v, 1, 0), ax, size))
                todo.append(((have(1),), ("rsend", p, st, v, 0, 1), ax, size))
                todo.append(((have(-1),), ("rsend", p, st, v, 1, 1), ax, size))
                todo.append(((have(1), ("rrecv", p, st, v, 0, 0)), ("rsend", p, st, v, 0, 2), ax, size))
                todo.append(((have(-1), ("rrecv", p, st, v, 1, 0)), ("rsend", p, st, v, 1, 2), ax, size))
                todo.append((
                    (have(0),) + tuple(("rrecv", p, st, v, w, q) for w in (0, 1) for q in (1, 2)),
                    ("own", p, st, v), None, 0,
                ))

    def pump():
        moved = True
        while moved:
            moved = False
            for entry in list(todo):
                needs, op, ax, size = entry
                if all(n in done for n in needs):
                    todo.remove(entry)
                    order.append(op)
                    if op[0] == "rsend":
                        _, p, st, v, way, kind = op
                        begin = max(free.get((ax, way), 0.0), t)
                        free[ax, way] = begin + size / RATE
                        arrive.append((free[ax, way] + LAT, ("rrecv", p, st, v, way, kind)))
                    else:
                        done.add(op)
                    moved = True
                    break

    while arrive or items or todo:
        arrive.sort()
        if arrive and (arrive[0][0] <= t or not items):
            at, op = arrive.pop(0)
            t = max(t, at) + T_EV
            done.add(op)
            order.append(op)
        else:
            item = items.pop(0)
            order.append(item)
            t += T_DN
            done.add(item)
        pump()
    return order, t


def kernel(
    tok, gain, ids, rw, wg, wu, wd, out, wdp,
    w0, w1, w2, g, acc, h, r1a, r1b, r2a, r2b, r3a, r3b,
    gs_sem, gr_sem, rs_sem, rr_sem, wl_sem, ws_sem, wr_sem, dl_sem,
):
    ws = (w0, w1, w2)
    ex, mp = lax.axis_index("expert"), lax.axis_index("mp")
    core, cy = lax.rem(ex, 2), lax.div(ex, 2)
    cx, cz = lax.rem(mp, 4), lax.div(mp, 4)
    me = (cz, cy, cx)
    pos = [[me[ax] if r == 0 else lax.rem(me[ax] + (r + 4) % 4, 4) for r in (0, 1, 2, -1)] for ax in range(3)]

    def at(ax, r):
        return pos[ax][r]

    def dev(ax, r):
        cc = [at(q, r if q == ax else 0) for q in range(3)]
        return (cc[1] * 2 + core, cc[0] * 4 + cc[2])

    other_core = (cy * 2 + (1 - core), mp)

    bar = pltpu.get_barrier_semaphore()
    for ax in range(3):
        for r in (1, -1):
            pl.semaphore_signal(bar, inc=1, device_id=dev(ax, r), device_id_type=MESH)
    pl.semaphore_signal(bar, inc=1, device_id=other_core, device_id_type=MESH)

    local_w = []
    for p in range(3):
        for q, src in ((0, wg), (1, wu)):
            cp = pltpu.make_async_copy(src.at[p], ws[p].at[:, :, :, :, :, pl.ds(q * F, F)], wl_sem.at[p, q])
            cp.start()
            local_w.append(cp)

    vals = tok[...].astype(jnp.float32)
    ms = jnp.mean(vals * vals, axis=1, keepdims=True)
    inv = lax.rsqrt(ms + 1e-05)
    scale = gain[...].astype(jnp.float32)
    for i in range(D // 128):
        piece = vals[:, i * 128:(i + 1) * 128] * inv * scale[i:i + 1, :]
        g[cz, cy, cx, :, pl.ds(i * 128, 128)] = piece.astype(jnp.bfloat16)
    lane = lax.broadcasted_iota(jnp.int32, (16, EXT), 1)
    diag = lax.broadcasted_iota(jnp.int32, (16, 16), 0) == lax.broadcasted_iota(jnp.int32, (16, 16), 1)

    def column(row):
        return jnp.sum(jnp.where(diag, row, 0.0), axis=1, keepdims=True)

    weights = rw[...]
    share = weights / (weights[0:1, :] + weights[1:2, :])
    which = ids[...].astype(jnp.float32)
    name = lax.rem(lane, 8).astype(jnp.float32)
    coef = jnp.where(name == column(which[0:1, :]), column(share[0:1, :]), 0.0)
    coef = coef + jnp.where(name == column(which[1:2, :]), column(share[1:2, :]), 0.0)
    hi = coef.astype(jnp.bfloat16).astype(jnp.float32)
    packed = jnp.where(lane < 8, hi, jnp.where(lane < 16, coef - hi, 0.0))
    g[cz, cy, cx, :, pl.ds(D, EXT)] = packed.astype(jnp.bfloat16)

    pl.semaphore_wait(bar, 7)

    def region(p, s, r, half):
        a, b, c = ORDER[p]
        idx = [None, None, None]
        if s == 0:
            idx[a], idx[b], idx[c] = at(a, r), at(b, 0), at(c, 0)
        elif s < 5:
            idx[a], idx[b], idx[c] = at(a, REL[s - 1]), at(b, r), at(c, 0)
        elif s < 9:
            idx[a], idx[b], idx[c] = at(a, REL[s - 5]), at(b, 0), at(c, r)
        else:
            idx[a], idx[b], idx[c] = slice(None), at(b, REL[s - 8]), at(c, r)
        lo, hi_ = p * PW, (p + 1) * PW + (EXT if p == 2 else 0)
        if half == 0:
            hi_ = lo + HW
        elif half == 1:
            lo = lo + HW
        return g.at[idx[0], idx[1], idx[2], :, pl.ds(lo, hi_ - lo)]

    def gcopy(p, s, k, sending):
        way = 1 if k % 2 == 0 else -1
        if sending:
            r = 0 if k < 2 else -way
        else:
            r = -way if k < 2 else 2
        reg = region(p, s, r, None if k < 2 else k - 2)
        ax = ORDER[p][axis_of(s)]
        return pltpu.make_async_remote_copy(
            src_ref=reg, dst_ref=reg, send_sem=gs_sem.at[p, s, k], recv_sem=gr_sem.at[p, s, k],
            device_id=dev(ax, way), device_id_type=MESH,
        )

    def wcopy(p, q):
        src = (wg, wu)[q]
        return pltpu.make_async_remote_copy(
            src_ref=src.at[p], dst_ref=ws[p].at[:, :, :, :, :, pl.ds(2 * F + q * F, F)],
            send_sem=ws_sem.at[p, q], recv_sem=wr_sem.at[p, q], device_id=other_core, device_id_type=MESH,
        )

    dcopy = pltpu.make_async_remote_copy(
        src_ref=wd, dst_ref=wdp, send_sem=ws_sem.at[3, 0], recv_sem=wr_sem.at[3, 0],
        device_id=other_core, device_id_type=MESH,
    )

    def plane(ax, r):
        return tuple(at(ax, r) if q == ax else slice(None) for q in range(3))

    def mm(p, n, j):
        cols = pl.ds(j * 2 * F, 2 * F)
        rhs = ws[p][:, :, :, :, :, cols].reshape(PW, 2 * F)
        if n in (0, 3):
            z, y, x = plane(ORDER[p][2], 0 if n == 0 else 2)
            lhs = g[z, y, x, :, pl.ds(p * PW, PW)].reshape(256, PW)
            res = jnp.dot(lhs, rhs, preferred_element_type=jnp.float32)
            acc[z, y, x, :, cols] += res.reshape(4, 4, 16, 2 * F)
            return
        pieces = []
        for v in REL[2 * n - 2:2 * n]:
            for r in (-1, 1):
                idx = [slice(None)] * 3
                idx[ORDER[p][1]], idx[ORDER[p][2]] = at(ORDER[p][1], v), at(ORDER[p][2], r)
                pieces.append(tuple(idx))
        lhs = jnp.concatenate([g[z, y, x, :, pl.ds(p * PW, PW)].reshape(64, PW) for z, y, x in pieces], axis=0)
        res = jnp.dot(lhs, rhs, preferred_element_type=jnp.float32)
        for i, (z, y, x) in enumerate(pieces):
            acc[z, y, x, :, cols] += res[64 * i:64 * i + 64].reshape(4, 16, 2 * F)

    def down(p, q):
        return pltpu.make_async_copy(
            (wd, wdp)[q].at[:, :, :, :, pl.ds(p * PW, PW)], ws[p].at[0, pl.ds(2 * q, 2)], dl_sem.at[p, q]
        )

    gather = plan_gather()[0]
    started = False
    have_w = set()
    for op in gather:
        if op[0] == "send":
            gcopy(*op[1:], True).start()
        elif op[0] == "recv":
            if not started:
                started = True
                for p in range(3):
                    for q in range(2):
                        wcopy(p, q).start()
                dcopy.start()
                acc[...] = jnp.zeros_like(acc)
            gcopy(*op[1:], False).wait_recv()
        elif op[0] == "wd":
            if op[1] == 0:
                dcopy.wait_recv()
            for q in range(2):
                down(op[1], q).start()
        else:
            _, p, n, j = op
            if (p, j) not in have_w:
                have_w.add((p, j))
                for q in range(2):
                    if j == 0:
                        local_w[p * 2 + q].wait()
                    else:
                        wcopy(p, q).wait_recv()
            mm(p, n, j)

    e_of = (ex, cy * 2 + (1 - core))

    def act(i, carry):
        z, y = lax.rem(cz + lax.div(i, 4), 4), lax.rem(i, 4)
        tile = g[z, y, :, :, pl.ds(D, EXT)].reshape(64, EXT).astype(jnp.float32)
        ln = lax.broadcasted_iota(jnp.int32, (64, EXT), 1)
        for j in range(2):
            mine = jnp.where((ln == e_of[j]) | (ln == e_of[j] + 8), tile, 0.0)
            cf = jnp.sum(mine, axis=1, keepdims=True)
            gate = acc[z, y, :, :, pl.ds(j * 2 * F, F)].reshape(64, F)
            up = acc[z, y, :, :, pl.ds(j * 2 * F + F, F)].reshape(64, F)
            res = gate / (1.0 + jnp.exp(-gate)) * up * cf
            h[z, y, :, :, pl.ds(j * F, F)] = res.astype(jnp.bfloat16).reshape(4, 16, F)
        return carry

    def dn(p, r):
        z, y, x = plane(ORDER[p][2], r)

        def tile(n, carry):
            cols = pl.ds(pl.multiple_of(n * HW, HW), HW)
            lhs = h[z, y, x].reshape(256, 2 * F)
            rhs = ws[p][0, :, :, :, :, cols].reshape(2 * F, HW)
            res = jnp.dot(lhs, rhs, preferred_element_type=jnp.float32)
            ws[p][1, z, y, x, :, cols] = res.astype(jnp.bfloat16).reshape(4, 4, 16, HW)
            return carry

        lax.fori_loop(0, 2, tile, 0)

    def part_region(p, st, v, r):
        a, b, c = ORDER[p]
        idx = [None, None, None]
        if st == 1:
            idx[a], idx[b], idx[c] = slice(None), at(b, v), at(c, r)
        elif st == 2:
            idx[a], idx[b], idx[c] = slice(None), at(b, r), at(c, 0)
        else:
            idx[a], idx[b], idx[c] = at(a, r), at(b, 0), at(c, 0)
        return tuple(idx)

    def half_cols(half):
        return pl.ds(half * HW, HW)

    def bufs(p, st, v, way):
        i = RS_SUB.index(v)
        if st == 1:
            return r1a.at[p, way, i], r1b.at[p, way, i]
        if st == 2:
            return r2a.at[p, way], r2b.at[p, way]
        return r3a.at[p, way], r3b.at[p, way]

    def slot(st, v):
        return RS_SUB.index(v) if st == 1 else st + 2

    def rcopy(p, st, v, way, kind):
        step = 1 if way == 0 else -1
        r = 2 if kind == 0 else step
        half = way if kind in (0, 2) else 1 - way
        z, y, x = part_region(p, st, v, r)
        src = ws[p].at[1, z, y, x, :, half_cols(half)]
        buf_a, buf_b = bufs(p, st, v, way)
        if kind == 0:
            dst = buf_a
        elif st == 3:
            dst = buf_b.at[:, half_cols(half)]
        else:
            dst = buf_b.at[:, :, half_cols(half)]
        return pltpu.make_async_remote_copy(
            src_ref=src, dst_ref=dst, send_sem=rs_sem.at[p, slot(st, v), way, kind],
            recv_sem=rr_sem.at[p, slot(st, v), way, kind],
            device_id=dev(ORDER[p][3 - st], step), device_id_type=MESH,
        )

    scatter = plan_scatter()[0]
    have_d = set()
    for op in scatter:
        if op[0] == "dn":
            _, p, r = op
            if p not in have_d:
                have_d.add(p)
                if p == 0:
                    lax.fori_loop(8, 12, act, 0)
                elif p == 1:
                    lax.fori_loop(0, 8, act, 0)
                    lax.fori_loop(12, 16, act, 0)
                down(p, 0).wait()
                down(p, 1).wait()
            dn(p, r)
        elif op[0] == "rsend":
            _, p, st, v, way, kind = op
            if kind == 2:
                z, y, x = part_region(p, st, v, 1 if way == 0 else -1)
                buf_a, _ = bufs(p, st, v, way)
                cols = half_cols(way)
                total = ws[p][1, z, y, x, :, cols].astype(jnp.float32) + buf_a[...].astype(jnp.float32)
                ws[p][1, z, y, x, :, cols] = total.astype(jnp.bfloat16)
            rcopy(p, st, v, way, kind).start()
        elif op[0] == "rrecv":
            rcopy(*op[1:]).wait_recv()
        else:
            _, p, st, v = op
            z, y, x = part_region(p, st, v, 0)
            b0, b1 = bufs(p, st, v, 0)[1], bufs(p, st, v, 1)[1]
            total = (
                ws[p][1, z, y, x].astype(jnp.float32) + b0[...].astype(jnp.float32) + b1[...].astype(jnp.float32)
            ).astype(jnp.bfloat16)
            if st == 3:
                out[:, pl.ds(p * PW, PW)] = total
            else:
                ws[p][1, z, y, x] = total

    for op in gather:
        if op[0] == "send":
            gcopy(*op[1:], True).wait_send()
    for op in scatter:
        if op[0] == "rsend":
            rcopy(*op[1:]).wait_send()
    for p in range(3):
        for q in range(2):
            wcopy(p, q).wait_send()
    dcopy.wait_send()


def local(tokens, norm_gain, expert_ids, slot_ids, route_weights, w_gate, w_up, w_down):
    bf = jnp.bfloat16
    vmem = pl.BlockSpec(memory_space=pltpu.VMEM)
    hbm = pl.BlockSpec(memory_space=pl.ANY)
    moe, _ = pl.pallas_call(
        kernel,
        name="moe",
        out_shape=(
            jax.ShapeDtypeStruct((16, D), bf),
            jax.ShapeDtypeStruct((2, 4, 4, 16, D), bf),
        ),
        in_specs=[vmem, vmem, vmem, vmem, hbm, hbm, hbm],
        out_specs=(vmem, hbm),
        scratch_shapes=[
            pltpu.VMEM((2, 4, 4, 4, 16, PW), bf),
            pltpu.VMEM((2, 4, 4, 4, 16, PW), bf),
            pltpu.VMEM((2, 4, 4, 4, 16, PW), bf),
            pltpu.VMEM((4, 4, 4, 16, D + EXT), bf),
            pltpu.VMEM((4, 4, 4, 16, 4 * F), jnp.float32),
            pltpu.VMEM((4, 4, 4, 16, 2 * F), bf),
            pltpu.VMEM((3, 2, 4, 4, 16, HW), bf),
            pltpu.VMEM((3, 2, 4, 4, 16, PW), bf),
            pltpu.VMEM((3, 2, 4, 16, HW), bf),
            pltpu.VMEM((3, 2, 4, 16, PW), bf),
            pltpu.VMEM((3, 2, 16, HW), bf),
            pltpu.VMEM((3, 2, 16, PW), bf),
            pltpu.SemaphoreType.DMA((3, 12, 4)),
            pltpu.SemaphoreType.DMA((3, 12, 4)),
            pltpu.SemaphoreType.DMA((3, 6, 2, 3)),
            pltpu.SemaphoreType.DMA((3, 6, 2, 3)),
            pltpu.SemaphoreType.DMA((3, 2)),
            pltpu.SemaphoreType.DMA((4, 2)),
            pltpu.SemaphoreType.DMA((4, 2)),
            pltpu.SemaphoreType.DMA((3, 2)),
        ],
        compiler_params=pltpu.CompilerParams(
            collective_id=0, has_side_effects=True, vmem_limit_bytes=67043328
        ),
    )(
        tokens,
        norm_gain.reshape(D // 128, 128),
        expert_ids.T,
        route_weights.T,
        w_gate.reshape(3, 2, 4, 4, 4, 16, F),
        w_up.reshape(3, 2, 4, 4, 4, 16, F),
        w_down.reshape(2, 4, 4, 16, D),
    )
    return moe


def solution(mesh):
    placed = (
        P(("expert", "mp"), None),
        P(),
        P(("expert", "mp"), None),
        P(("expert", "mp"), None),
        P(("expert", "mp"), None),
        P("expert", None, "mp"),
        P("expert", None, "mp"),
        P("expert", "mp", None),
    )
    return jax.shard_map(
        local, mesh=mesh, in_specs=placed, out_specs=P(("expert", "mp"), None), check_vma=False
    )
```
